8 devices in a mesh: dp: 2 (over z, y), sp: 4 (over x, core).
Axes of the slice: x: 2, y: 2, z: 1, core: 2. Of those that a mesh axis runs over, the one named last changes fastest.
Arguments:
- x: bfloat16 [2, 4096, 4096], P('dp', 'sp'), parts along dimension 0
- segment_ids: int32 [2, 4096], P('dp', 'sp'), parts along dimension 0
- positions: int32 [2, 4096], P('dp', 'sp'), parts along dimension 0
- out_grad: bfloat16 [2, 4096, 4096], P('dp', 'sp'), parts along dimension 0
- norm_scale: bfloat16 [4096], replicated
- w_q: bfloat16 [4096, 4096], replicated
- w_k: bfloat16 [4096, 256], replicated
- w_v: bfloat16 [4096, 256], replicated
- w_o: bfloat16 [4096, 4096], replicated
- b_o: bfloat16 [4096], replicated
Outputs:
- output 1: bfloat16 [2, 4096, 4096], P('dp', 'sp'), parts along dimension 0
- output 2: bfloat16 [2, 4096, 4096], P('dp', 'sp'), parts along dimension 0
- output 3: bfloat16 [8192], P('dp'), parts along dimension 0
- output 4: bfloat16 [8192, 4096], P('dp'), parts along dimension 0
- output 5: bfloat16 [8192, 256], P('dp'), parts along dimension 0
- output 6: bfloat16 [8192, 256], P('dp'), parts along dimension 0
- output 7: bfloat16 [8192, 4096], P('dp'), parts along dimension 0
- output 8: bfloat16 [8192], P('dp'), parts along dimension 0
There are 2 independent parts. The reference program is written for one: setup_inputs(seed, part) draws one part's arguments, and reference() takes and returns one part's arrays. A program takes and returns all parts, laid end to end along the dimension named above; an argument that names none is the same for every part.
All inputs are finite; a program needn't handle non-finite values.
Results may differ from the reference program's by a relative error of at most 0.017504.
Values are sent between devices in bfloat16 or wider.
A program may use at most 1 GiB of HBM per device.

```python
import jax
import jax.numpy as jnp
from jax import lax

BATCH_SIZE = 1
SEQ_LEN = 4096
MODEL_DIM = 4096
NUM_HEADS = 16
HEAD_DIM = 256
WINDOW = 2048
QUERY_BLOCK = 128
DOC_MEAN = max(QUERY_BLOCK, min(2 * WINDOW, SEQ_LEN // 4))
QK_GAIN = 1.7
NORM_EPS = 1e-6
ROPE_BASE = 10000.0
NEG_BIG = -1e30


def draw_documents(start_key, offset_key):
    token_idx = jnp.arange(SEQ_LEN, dtype=jnp.int32)[None, :]
    starts = jax.random.randint(start_key, (BATCH_SIZE, SEQ_LEN), 0, DOC_MEAN) == 0
    starts = starts & (token_idx > 0)
    seg_ids = jnp.cumsum(starts.astype(jnp.int32), axis=1).astype(jnp.int32)
    doc_start = lax.cummax(jnp.where(starts, token_idx, 0), axis=1)
    row_offset = jax.random.randint(offset_key, (BATCH_SIZE, 1), 0, 4096)
    positions = (token_idx - doc_start + row_offset).astype(jnp.int32)
    return seg_ids, positions


def setup_inputs(seed: int = 0, part: int = 0) -> dict:
    shared_keys = jax.random.split(jax.random.key(seed), 7)
    part_keys = jax.random.split(jax.random.fold_in(jax.random.key(seed + 1), part), 4)
    seg_ids, positions = draw_documents(part_keys[2], part_keys[3])
    act_shape = (BATCH_SIZE, SEQ_LEN, MODEL_DIM)
    q_width = NUM_HEADS * HEAD_DIM
    in_std = MODEL_DIM ** -0.5

    def normal_bf16(rng_key, shape, std_dev):
        return (jax.random.normal(rng_key, shape, jnp.float32) * std_dev).astype(jnp.bfloat16)

    return {
        "x": normal_bf16(part_keys[0], act_shape, 1.0),
        "segment_ids": seg_ids,
        "positions": positions,
        "out_grad": normal_bf16(part_keys[1], act_shape, 1.0),
        "norm_scale": normal_bf16(shared_keys[0], (MODEL_DIM,), 0.3),
        "w_q": normal_bf16(shared_keys[1], (MODEL_DIM, q_width), QK_GAIN * in_std),
        "w_k": normal_bf16(shared_keys[2], (MODEL_DIM, HEAD_DIM), QK_GAIN * in_std),
        "w_v": normal_bf16(shared_keys[3], (MODEL_DIM, HEAD_DIM), in_std),
        "w_o": normal_bf16(shared_keys[4], (q_width, MODEL_DIM), q_width ** -0.5),
        "b_o": normal_bf16(shared_keys[5], (MODEL_DIM,), 0.3),
    }


def rms_norm(x_f32, norm_gain):
    mean_sq = jnp.mean(x_f32 * x_f32, axis=-1, keepdims=True)
    return (x_f32 * lax.rsqrt(mean_sq + NORM_EPS) * (1.0 + norm_gain.astype(jnp.float32))).astype(jnp.bfloat16)


def rotary(head_vals, positions):
    rot_dim = HEAD_DIM // 2
    half_dim = rot_dim // 2
    inv_freq = ROPE_BASE ** (-(jnp.arange(half_dim, dtype=jnp.float32) * 2.0 / rot_dim))
    angles = positions.astype(jnp.float32)[:, :, None, None] * inv_freq
    cos_a = jnp.cos(angles)
    sin_a = jnp.sin(angles)
    first_half = head_vals[..., :half_dim]
    second_half = head_vals[..., half_dim:rot_dim]
    return jnp.concatenate([first_half * cos_a - second_half * sin_a, second_half * cos_a + first_half * sin_a, head_vals[..., rot_dim:]], axis=-1)


def attention(queries, keys_in, values_in, seg_ids):
    batch_rows, seq_len, n_heads, head_dim = queries.shape
    key_span = WINDOW + QUERY_BLOCK
    keys_pad = jnp.pad(keys_in, ((0, 0), (WINDOW, 0), (0, 0)))
    values_pad = jnp.pad(values_in, ((0, 0), (WINDOW, 0), (0, 0)))
    seg_pad = jnp.pad(seg_ids, ((0, 0), (WINDOW, 0)), constant_values=-1)
    offsets = jnp.arange(key_span)[None, :]
    row_idx = jnp.arange(QUERY_BLOCK)[:, None]
    in_band = (offsets > row_idx) & (offsets <= row_idx + WINDOW)

    def one_block(q_start):
        q_blk = lax.dynamic_slice_in_dim(queries, q_start, QUERY_BLOCK, axis=1)
        k_blk = lax.dynamic_slice_in_dim(keys_pad, q_start, key_span, axis=1)
        v_blk = lax.dynamic_slice_in_dim(values_pad, q_start, key_span, axis=1)
        q_seg = lax.dynamic_slice_in_dim(seg_ids, q_start, QUERY_BLOCK, axis=1)
        k_seg = lax.dynamic_slice_in_dim(seg_pad, q_start, key_span, axis=1)
        allowed = (q_seg[:, :, None] == k_seg[:, None, :]) & in_band[None]
        scores = jnp.einsum("bqhe,bke->bhqk", q_blk.astype(jnp.float32), k_blk.astype(jnp.float32))
        scores = jnp.where(allowed[:, None], scores, NEG_BIG)
        attn_prob = jax.nn.softmax(scores, axis=-1).astype(jnp.bfloat16)
        o_blk = jnp.einsum("bhqk,bke->bqhe", attn_prob.astype(jnp.float32), v_blk.astype(jnp.float32))
        return o_blk.astype(jnp.bfloat16)

    blocks = lax.map(jax.checkpoint(one_block), jnp.arange(seq_len // QUERY_BLOCK) * QUERY_BLOCK)
    return jnp.moveaxis(blocks, 0, 1).reshape(batch_rows, seq_len, n_heads, head_dim)


def forward(x, norm_scale, w_q, w_k, w_v, w_o, b_o, seg_ids, positions):
    x_f32 = x.astype(jnp.float32)
    normed = rms_norm(x_f32, norm_scale)
    q_lin = jnp.dot(normed, w_q, preferred_element_type=jnp.float32).reshape(BATCH_SIZE, SEQ_LEN, NUM_HEADS, HEAD_DIM)
    queries = (rotary(q_lin, positions) * HEAD_DIM ** -0.5).astype(jnp.bfloat16)
    keys_all = rotary(jnp.dot(normed, w_k, preferred_element_type=jnp.float32)[:, :, None, :], positions)[:, :, 0, :].astype(jnp.bfloat16)
    values_all = jnp.dot(normed, w_v, preferred_element_type=jnp.float32).astype(jnp.bfloat16)
    attn_out = attention(queries, keys_all, values_all, seg_ids)
    y_proj = jnp.dot(attn_out.reshape(BATCH_SIZE, SEQ_LEN, NUM_HEADS * HEAD_DIM), w_o, preferred_element_type=jnp.float32)
    return (x_f32 + y_proj + b_o.astype(jnp.float32)).astype(jnp.bfloat16)


def reference(x, segment_ids, positions, out_grad, norm_scale, w_q, w_k, w_v, w_o, b_o):
    def block_fn(x_in, gain_in, wq_in, wk_in, wv_in, wo_in, bo_in):
        return forward(x_in, gain_in, wq_in, wk_in, wv_in, wo_in, bo_in, segment_ids, positions)

    block_out, pull_back = jax.vjp(block_fn, x, norm_scale, w_q, w_k, w_v, w_o, b_o)
    all_grads = pull_back(out_grad)
    return (block_out, all_grads[0], all_grads[1], all_grads[2], all_grads[3], all_grads[4], all_grads[5], all_grads[6])
```

```python
import functools

import jax
import jax.numpy as jnp
from jax import lax
from jax.experimental import pallas as pl
from jax.experimental.pallas import tpu as pltpu
from jax.sharding import PartitionSpec as P

WINDOW = 2048
NORM_EPS = 1e-6
ROPE_BASE = 10000.0
NEG_BIG = -1e30
POS_BIG = 3e38
HEAD_DIM = 256
ROT_HALF = HEAD_DIM // 4

FWD_BQ, FWD_BK, FWD_G = 256, 512, 4
BWD_BQ, BWD_BK, BWD_G = 256, 512, 4

NT = (((1,), (1,)), ((), ()))
NN = (((1,), (0,)), ((), ()))


def dot(a, b, dims):
    return lax.dot_general(a, b, dims, preferred_element_type=jnp.float32)


def rms_norm(x_f32, gain_f32):
    mean_sq = jnp.mean(x_f32 * x_f32, axis=-1, keepdims=True)
    return (x_f32 * lax.rsqrt(mean_sq + NORM_EPS) * (1.0 + gain_f32)).astype(jnp.bfloat16)


def rope_tables(positions):
    rot_dim = 2 * ROT_HALF
    inv_freq = ROPE_BASE ** (-(jnp.arange(ROT_HALF, dtype=jnp.float32) * 2.0 / rot_dim))
    angles = positions.astype(jnp.float32)[:, None] * inv_freq
    return jnp.cos(angles), jnp.sin(angles)


def rotary(vals, cos_a, sin_a):
    a = vals[..., :ROT_HALF]
    b = vals[..., ROT_HALF:2 * ROT_HALF]
    cos_a, sin_a = cos_a[:, None, :], sin_a[:, None, :]
    return jnp.concatenate([a * cos_a - b * sin_a, b * cos_a + a * sin_a, vals[..., 2 * ROT_HALF:]], axis=-1)


def key_cap(k0, first_key, own_key, bk, bq):
    key_idx = k0 + lax.broadcasted_iota(jnp.int32, (bk, bq), 0)
    return jnp.where((key_idx >= first_key) & (key_idx <= own_key), POS_BIG, NEG_BIG)


def fwd_kernel(bq, bk, group, lo_ref, hi_ref, t0_ref, q_ref, k_ref, vt_ref, first_ref, o_ref, lse_ref, m_s, l_s, acc_s):
    i = pl.program_id(0)
    first_key = first_ref[0]
    own_key = t0_ref[i] + lax.broadcasted_iota(jnp.int32, (1, bq), 1)
    m_s[...] = jnp.full_like(m_s, NEG_BIG)
    l_s[...] = jnp.zeros_like(l_s)
    acc_s[...] = jnp.zeros_like(acc_s)

    def body(j, carry):
        k0 = pl.multiple_of(j * bk, bk)
        k_blk = k_ref[pl.ds(k0, bk), :]
        vt_blk = vt_ref[:, pl.ds(k0, bk)]
        cap = key_cap(k0, first_key, own_key, bk, bq)
        for h in range(group):
            s = jnp.minimum(dot(k_blk, q_ref[:, h * HEAD_DIM:(h + 1) * HEAD_DIM], NT), cap)
            m_old = m_s[h:h + 1]
            m_new = jnp.maximum(m_old, jnp.max(s, axis=0, keepdims=True))
            p = jnp.exp(s - m_new)
            alpha = jnp.exp(m_old - m_new)
            l_s[h:h + 1] = l_s[h:h + 1] * alpha + jnp.sum(p, axis=0, keepdims=True)
            m_s[h:h + 1] = m_new
            acc_s[h] = acc_s[h] * alpha + dot(vt_blk, p.astype(jnp.bfloat16), NN)
        return carry

    lax.fori_loop(lo_ref[i], hi_ref[i], body, 0)
    for h in range(group):
        l_h = l_s[h:h + 1]
        o_ref[:, h * HEAD_DIM:(h + 1) * HEAD_DIM] = (acc_s[h] / l_h).T.astype(jnp.bfloat16)
        lse_ref[0, 0, h:h + 1] = m_s[h:h + 1] + jnp.log(l_h)


def block_bounds(first_key, t0, bq, bk):
    blk_first = first_key.reshape(-1, bq)[:, 0]
    starts = t0 + jnp.arange(first_key.shape[0] // bq, dtype=jnp.int32) * bq
    return blk_first // bk, (starts + bq - 1) // bk + 1, starts


def attn_fwd(q, k, vt, first_key, t0):
    bq, bk, group = FWD_BQ, FWD_BK, FWD_G
    tokens, width = q.shape
    seq = k.shape[0]
    nq, ng = tokens // bq, width // (group * HEAD_DIM)
    lo, hi, starts = block_bounds(first_key, t0, bq, bk)
    o, lse = pl.pallas_call(
        functools.partial(fwd_kernel, bq, bk, group),
        grid_spec=pltpu.PrefetchScalarGridSpec(
            num_scalar_prefetch=3, grid=(nq, ng),
            in_specs=[pl.BlockSpec((bq, group * HEAD_DIM), lambda i, g, *_: (i, g)),
                      pl.BlockSpec((seq, HEAD_DIM), lambda i, g, *_: (0, 0)),
                      pl.BlockSpec((HEAD_DIM, seq), lambda i, g, *_: (0, 0)),
                      pl.BlockSpec((1, 1, bq), lambda i, g, *_: (i, 0, 0))],
            out_specs=[pl.BlockSpec((bq, group * HEAD_DIM), lambda i, g, *_: (i, g)),
                       pl.BlockSpec((1, 1, group, bq), lambda i, g, *_: (i, g, 0, 0))],
            scratch_shapes=[pltpu.VMEM((group, bq), jnp.float32), pltpu.VMEM((group, bq), jnp.float32),
                            pltpu.VMEM((group, HEAD_DIM, bq), jnp.float32)]),
        out_shape=[jax.ShapeDtypeStruct(q.shape, jnp.bfloat16),
                   jax.ShapeDtypeStruct((nq, ng, group, bq), jnp.float32)],
        compiler_params=pltpu.CompilerParams(dimension_semantics=("arbitrary", "arbitrary")),
        cost_estimate=pl.CostEstimate(flops=4 * tokens * width * 1024, bytes_accessed=4 * tokens * width, transcendentals=0),
        name="attn_fwd",
    )(lo, hi, starts, q, k, vt, first_key.reshape(nq, 1, bq))
    return o, lse


def bwd_kernel(bq, bk, group, lo_ref, hi_ref, t0_ref, q_ref, do_ref, o_ref, lse_ref, first_ref, cos_ref, sin_ref,
               k_ref, kt_ref, v_ref, dk_in, dv_in, dq_ref, dk_ref, dv_ref, dq_s, delta_s):
    i = pl.program_id(0)

    @pl.when((i == 0) & (pl.program_id(1) == 0))
    def _():
        dk_ref[...] = dk_in[...]
        dv_ref[...] = dv_in[...]

    first_key = first_ref[0]
    own_key = t0_ref[i] + lax.broadcasted_iota(jnp.int32, (1, bq), 1)
    dq_s[...] = jnp.zeros_like(dq_s)
    for h in range(group):
        cols = slice(h * HEAD_DIM, (h + 1) * HEAD_DIM)
        row_dot = jnp.sum(do_ref[:, cols].astype(jnp.float32) * o_ref[:, cols].astype(jnp.float32), axis=1, keepdims=True)
        delta_s[h:h + 1] = jnp.broadcast_to(row_dot, (bq, 128)).T[0:1]

    def body(j, carry):
        k0 = pl.multiple_of(j * bk, bk)
        k_blk = k_ref[pl.ds(k0, bk), :]
        v_blk = v_ref[pl.ds(k0, bk), :]
        kt_blk = kt_ref[:, pl.ds(k0, bk)]
        cap = key_cap(k0, first_key, own_key, bk, bq)
        p_all, ds_all = [], []
        for h in range(group):
            cols = slice(h * HEAD_DIM, (h + 1) * HEAD_DIM)
            s = jnp.minimum(dot(k_blk, q_ref[:, cols], NT), cap)
            p = jnp.exp(s - lse_ref[0, 0, h:h + 1])
            dp = dot(v_blk, do_ref[:, cols], NT)
            ds = (p * (dp - delta_s[h:h + 1])).astype(jnp.bfloat16)
            p_all.append(p.astype(jnp.bfloat16))
            ds_all.append(ds)
            dq_s[h] += dot(kt_blk, ds, NN)
        q_rows = jnp.concatenate([q_ref[:, h * HEAD_DIM:(h + 1) * HEAD_DIM] for h in range(group)], axis=0)
        do_rows = jnp.concatenate([do_ref[:, h * HEAD_DIM:(h + 1) * HEAD_DIM] for h in range(group)], axis=0)
        dv_ref[pl.ds(k0, bk), :] += dot(jnp.concatenate(p_all, axis=1), do_rows, NN)
        dk_ref[pl.ds(k0, bk), :] += dot(jnp.concatenate(ds_all, axis=1), q_rows, NN)
        return carry

    lax.fori_loop(lo_ref[i], hi_ref[i], body, 0)
    cos_t, sin_t = cos_ref[...], sin_ref[...]
    for h in range(group):
        dq = dq_s[h].astype(jnp.bfloat16).astype(jnp.float32)
        a, b = dq[:ROT_HALF], dq[ROT_HALF:2 * ROT_HALF]
        dq_lin = jnp.concatenate([a * cos_t + b * sin_t, b * cos_t - a * sin_t, dq[2 * ROT_HALF:]], axis=0) * HEAD_DIM ** -0.5
        dq_ref[:, h * HEAD_DIM:(h + 1) * HEAD_DIM] = dq_lin.T.astype(jnp.bfloat16)


def attn_bwd(q, d_o, o, lse, k, kt, v, first_key, t0, cos_a, sin_a, dk_in, dv_in):
    bq, bk, group = BWD_BQ, BWD_BK, BWD_G
    tokens, width = q.shape
    seq = k.shape[0]
    nq, ng = tokens // bq, width // (group * HEAD_DIM)
    lo, hi, starts = block_bounds(first_key, t0, bq, bk)
    tile = pl.BlockSpec((bq, group * HEAD_DIM), lambda i, g, *_: (i, g))
    whole = pl.BlockSpec((seq, HEAD_DIM), lambda i, g, *_: (0, 0))
    trig = pl.BlockSpec((ROT_HALF, bq), lambda i, g, *_: (0, i))
    acc_shape = jax.ShapeDtypeStruct((seq, HEAD_DIM), jnp.float32)
    return pl.pallas_call(
        functools.partial(bwd_kernel, bq, bk, group),
        grid_spec=pltpu.PrefetchScalarGridSpec(
            num_scalar_prefetch=3, grid=(nq, ng),
            in_specs=[tile, tile, tile,
                      pl.BlockSpec((1, 1, group, bq), lambda i, g, *_: (i, g, 0, 0)),
                      pl.BlockSpec((1, 1, bq), lambda i, g, *_: (i, 0, 0)),
                      trig, trig, whole, pl.BlockSpec((HEAD_DIM, seq), lambda i, g, *_: (0, 0)), whole, whole, whole],
            out_specs=[tile, whole, whole],
            scratch_shapes=[pltpu.VMEM((group, HEAD_DIM, bq), jnp.float32), pltpu.VMEM((group, bq), jnp.float32)]),
        out_shape=[jax.ShapeDtypeStruct(q.shape, jnp.bfloat16), acc_shape, acc_shape],
        compiler_params=pltpu.CompilerParams(dimension_semantics=("arbitrary", "arbitrary"), vmem_limit_bytes=60 * 2 ** 20),
        cost_estimate=pl.CostEstimate(flops=10 * tokens * width * 1024, bytes_accessed=8 * tokens * width, transcendentals=0),
        name="attn_bwd",
    )(lo, hi, starts, q, d_o, o, lse, first_key.reshape(nq, 1, bq), cos_a.T, sin_a.T, k, kt, v, dk_in, dv_in)


def solution(mesh):
    row_spec = P("dp", "sp", None)
    tok_spec = P("dp", "sp")
    mat_spec = P(None, None)
    grad_mat = P("dp", None)
    chips_perm = [(0, 2), (1, 3), (2, 0), (3, 1)]
    cores_perm = [(0, 1), (1, 0), (2, 3), (3, 2)]

    def to_chip(val):
        return lax.ppermute(val, "sp", chips_perm)

    def to_core(val):
        return lax.ppermute(val, "sp", cores_perm)

    def by_core(core, mine, theirs, axis):
        first = jnp.where(core == 0, mine, theirs)
        second = jnp.where(core == 0, theirs, mine)
        return jnp.concatenate([first, second], axis=axis)

    def local_step(x, seg_ids, positions, out_grad, norm_scale, w_q, w_k, w_v, w_o, b_o):
        x, out_grad = x[0], out_grad[0]
        chunk, dim = x.shape
        me = lax.axis_index("sp")
        core = me % 2
        half = w_q.shape[1] // 2
        pieces = [me, me ^ 1, me ^ 2, me ^ 3]

        meta = lax.all_gather(jnp.stack([seg_ids[0], positions[0]]), "sp", axis=1, tiled=True)
        seg_all, pos_all = meta[0], meta[1]
        seq = seg_all.shape[0]
        token = jnp.arange(seq, dtype=jnp.int32)
        is_start = jnp.concatenate([jnp.ones((1,), jnp.bool_), seg_all[1:] != seg_all[:-1]])
        doc_start = lax.cummax(jnp.where(is_start, token, 0))
        first_key_all = jnp.maximum(doc_start, token - (WINDOW - 1))
        cos_all, sin_all = rope_tables(pos_all)

        def piece_rows(val, piece):
            return lax.dynamic_slice_in_dim(val, piece * chunk, chunk, axis=0)

        x_f32 = x.astype(jnp.float32)
        n_own, norm_pull = jax.vjp(rms_norm, x_f32, norm_scale.astype(jnp.float32))

        w_kv = jnp.concatenate([w_k, w_v], axis=1)
        kv_lin = dot(n_own, w_kv, NN)
        cos_own, sin_own = piece_rows(cos_all, me), piece_rows(sin_all, me)
        k_own = rotary(kv_lin[:, None, :HEAD_DIM], cos_own, sin_own)[:, 0].astype(jnp.bfloat16)
        kv_own = jnp.concatenate([k_own, kv_lin[:, HEAD_DIM:].astype(jnp.bfloat16)], axis=1)
        kv_1 = to_core(kv_own)
        kv_2 = to_chip(kv_own)
        kv_3 = to_core(kv_2)
        kv_all = jnp.zeros((seq, 2 * HEAD_DIM), jnp.bfloat16)
        for piece, val in zip(pieces, (kv_own, kv_1, kv_2, kv_3)):
            kv_all = lax.dynamic_update_slice_in_dim(kv_all, val, piece * chunk, axis=0)
        k_all, v_all = kv_all[:, :HEAD_DIM], kv_all[:, HEAD_DIM:]
        kt_all, vt_all = k_all.T, v_all.T

        n_1 = to_core(n_own)
        n_2 = to_chip(n_own)
        n_3 = to_core(n_2)
        g_1 = to_core(out_grad)
        g_2 = to_chip(out_grad)
        g_3 = to_core(g_2)
        n_all = [n_own, n_1, n_2, n_3]
        g_all = [out_grad, g_1, g_2, g_3]

        w_q_half = lax.dynamic_slice_in_dim(w_q, core * half, half, axis=1)
        w_o_half = lax.dynamic_slice_in_dim(w_o, core * half, half, axis=0)

        o_all, dq_all = [], []
        dk = jnp.zeros((seq, HEAD_DIM), jnp.float32)
        dv = jnp.zeros((seq, HEAD_DIM), jnp.float32)
        for p in range(4):
            first_key = piece_rows(first_key_all, pieces[p])
            cos_p, sin_p = piece_rows(cos_all, pieces[p]), piece_rows(sin_all, pieces[p])
            q_lin = dot(n_all[p], w_q_half, NN).reshape(chunk, -1, HEAD_DIM)
            q = (rotary(q_lin, cos_p, sin_p) * HEAD_DIM ** -0.5).astype(jnp.bfloat16).reshape(chunk, half)
            o, lse = attn_fwd(q, k_all, vt_all, first_key, pieces[p] * chunk)
            d_o = dot(g_all[p], w_o_half, NT).astype(jnp.bfloat16)
            dq, dk, dv = attn_bwd(q, d_o, o, lse, k_all, kt_all, v_all, first_key, pieces[p] * chunk, cos_p, sin_p, dk, dv)
            o_all.append(o)
            dq_all.append(dq)

        o_tok = by_core(core, o_all[0], to_core(o_all[1]), 1)
        block_out = (x_f32 + dot(o_tok, w_o, NN) + b_o.astype(jnp.float32)).astype(jnp.bfloat16)

        TN = (((0,), (0,)), ((), ()))
        w_o_part = sum(dot(o_all[p], g_all[p], TN) for p in range(4)).astype(jnp.bfloat16)
        w_q_part = sum(dot(n_all[p], dq_all[p], TN) for p in range(4)).astype(jnp.bfloat16)
        w_o_grad = by_core(core, w_o_part, to_core(w_o_part), 0)
        w_q_grad = by_core(core, w_q_part, to_core(w_q_part), 1)

        dkv = jnp.concatenate([dk, dv], axis=1)
        dkv = dkv + to_core(dkv)
        dk_lin = rotary(dkv[:, None, :HEAD_DIM].astype(jnp.bfloat16).astype(jnp.float32), cos_all, -sin_all)[:, 0].astype(jnp.bfloat16)
        dkv_lin = jnp.concatenate([dk_lin, dkv[:, HEAD_DIM:].astype(jnp.bfloat16)], axis=1)
        w_kv_grad = sum(dot(n_all[p], piece_rows(dkv_lin, pieces[p]), TN) for p in range(4)).astype(jnp.bfloat16)

        dq_tok = by_core(core, dq_all[0], to_core(dq_all[1]), 1)
        d_normed = (dot(dq_tok, w_q, NT) + dot(piece_rows(dkv_lin, me), w_kv, NT)).astype(jnp.bfloat16)
        dx_norm, gain_part = norm_pull(d_normed)
        x_grad = (out_grad.astype(jnp.float32) + dx_norm).astype(jnp.bfloat16)
        b_o_part = jnp.sum(out_grad, axis=0, dtype=jnp.float32)
        sums = lax.psum(jnp.stack([gain_part, b_o_part]), "sp").astype(jnp.bfloat16)
        return (block_out[None], x_grad[None], sums[0], w_q_grad, w_kv_grad[:, :HEAD_DIM], w_kv_grad[:, HEAD_DIM:], w_o_grad, sums[1])

    return jax.shard_map(local_step, mesh=mesh,
                         in_specs=(row_spec, tok_spec, tok_spec, row_spec, P(None), mat_spec, mat_spec, mat_spec, mat_spec, P(None)),
                         out_specs=(row_spec, row_spec, P("dp"), grad_mat, grad_mat, grad_mat, grad_mat, P("dp")),
                         check_vma=False)
```

```python
import functools

import jax
import jax.numpy as jnp
from jax import lax
from jax.experimental import pallas as pl
from jax.experimental.pallas import tpu as pltpu
from jax.sharding import PartitionSpec as P


WINDOW = 2048
NORM_EPS = 1e-6
ROPE_BASE = 10000.0
NEG_BIG = -1e30
POS_BIG = 3e38
HEAD_DIM = 256
ROT_HALF = HEAD_DIM // 4

FWD_BQ, FWD_BK = 256, 512
BWD_BQ, BWD_BK = 512, 512
VMEM_LIMIT = 67043328

NT = (((1,), (1,)), ((), ()))
NN = (((1,), (0,)), ((), ()))
TN = (((0,), (0,)), ((), ()))


def dot(a, b, dims):
    return lax.dot_general(a, b, dims, preferred_element_type=jnp.float32)


def rms_norm(x_f32, gain_f32):
    mean_sq = jnp.mean(x_f32 * x_f32, axis=-1, keepdims=True)
    return (x_f32 * lax.rsqrt(mean_sq + NORM_EPS) * (1.0 + gain_f32)).astype(jnp.bfloat16)


def rope_tables(positions):
    rot_dim = 2 * ROT_HALF
    inv_freq = ROPE_BASE ** (-(jnp.arange(ROT_HALF, dtype=jnp.float32) * 2.0 / rot_dim))
    angles = positions.astype(jnp.float32)[:, None] * inv_freq
    return jnp.cos(angles), jnp.sin(angles)


def rotary(vals, cos_a, sin_a):
    a = vals[..., :ROT_HALF]
    b = vals[..., ROT_HALF:2 * ROT_HALF]
    cos_a, sin_a = cos_a[:, None, :], sin_a[:, None, :]
    return jnp.concatenate([a * cos_a - b * sin_a, b * cos_a + a * sin_a, vals[..., 2 * ROT_HALF:]], axis=-1)


def resident(shape):
    return pl.BlockSpec(shape, lambda *_: (0,) * len(shape), pipeline_mode=pl.Buffered(1))


def params(axes, **kwargs):
    return pltpu.CompilerParams(dimension_semantics=("arbitrary",) * axes, vmem_limit_bytes=VMEM_LIMIT, **kwargs)


def proj_kernel(dims, rope, core_ref, a0_ref, a1_ref, w_ref, *rest):
    out_ref = rest[-1]
    rows = a0_ref.shape[0]
    for piece, a_ref in enumerate((a0_ref, a1_ref)):
        y = dot(a_ref[...], w_ref[...], dims)
        r = slice(piece * rows, (piece + 1) * rows)
        if not rope:
            out_ref[r, :] = y.astype(jnp.bfloat16)
            continue
        cos_a, sin_a = rest[0][r, :], rest[1][r, :]
        for h in range(y.shape[1] // HEAD_DIM):
            c0, c1, c2 = h * HEAD_DIM, h * HEAD_DIM + 2 * ROT_HALF, (h + 1) * HEAD_DIM
            turned = y[:, c0:c1] * cos_a + pltpu.roll(y[:, c0:c1], ROT_HALF, 1) * sin_a
            out_ref[r, c0:c1] = (turned * HEAD_DIM ** -0.5).astype(jnp.bfloat16)
            out_ref[r, c1:c2] = (y[:, c1:c2] * HEAD_DIM ** -0.5).astype(jnp.bfloat16)


def proj_pair(a0, a1, w, core, by_rows, tables=()):
    rows, depth = a0.shape
    half = w.shape[0 if by_rows else 1] // 2
    bn = 512
    nb = half // bn
    if by_rows:
        w_spec = pl.BlockSpec((bn, depth), lambda j, c: (c[0] * nb + j, 0))
    else:
        w_spec = pl.BlockSpec((depth, bn), lambda j, c: (0, c[0] * nb + j))
    return pl.pallas_call(
        functools.partial(proj_kernel, NT if by_rows else NN, bool(tables)),
        grid_spec=pltpu.PrefetchScalarGridSpec(
            num_scalar_prefetch=1, grid=(nb,),
            in_specs=[resident(a0.shape), resident(a1.shape), w_spec] + [resident(t.shape) for t in tables],
            out_specs=pl.BlockSpec((2 * rows, bn), lambda j, c: (0, j))),
        out_shape=jax.ShapeDtypeStruct((2 * rows, half), jnp.bfloat16),
        compiler_params=params(1),
        cost_estimate=pl.CostEstimate(flops=4 * rows * depth * half, bytes_accessed=2 * (2 * rows * (depth + half) + depth * half), transcendentals=0),
        name="proj_pair",
    )(core, a0, a1, w, *tables)


def wgrad_kernel(pieces, whole, col_sum, carried, core_ref, *refs):
    a_refs, b_refs, outs = refs[:pieces], refs[pieces:2 * pieces], refs[2 * pieces:]
    if carried:
        outs[-1][...] = outs[0][...]
        outs = outs[2:-1]
    y = sum(dot(a[...], b[...], TN) for a, b in zip(a_refs, b_refs)).astype(jnp.bfloat16)
    outs[0][...] = y
    if whole:
        outs[1][...] = y
    if col_sum:
        @pl.when(pl.program_id(0) == 0)
        def _():
            outs[-1][...] = sum(jnp.sum(b[...].astype(jnp.float32), axis=0, keepdims=True) for b in b_refs)


def wgrad(a, b, core, rows, bm, bn, whole_axis=None, col_sum=False, carried=()):
    m, n = a[0][0].shape[1], b[0][0].shape[1]
    mb, nb = m // bm, n // bn
    out_specs = [pl.BlockSpec((bm, bn), lambda i, j, c: (i, j))]
    out_shape = [jax.ShapeDtypeStruct((m, n), jnp.bfloat16)]
    if whole_axis == 0:
        out_specs.append(pl.BlockSpec((bm, bn), lambda i, j, c: (c[0] * mb + i, j)))
        out_shape.append(jax.ShapeDtypeStruct((2 * m, n), jnp.bfloat16))
    if whole_axis == 1:
        out_specs.append(pl.BlockSpec((bm, bn), lambda i, j, c: (i, c[0] * nb + j)))
        out_shape.append(jax.ShapeDtypeStruct((m, 2 * n), jnp.bfloat16))
    if col_sum:
        out_specs.append(pl.BlockSpec((1, bn), lambda i, j, c: (0, jnp.where(i == 0, j, nb - 1))))
        out_shape.append(jax.ShapeDtypeStruct((1, n), jnp.float32))
    extra_specs, aliases = [], {}
    if carried:
        steps = mb * nb
        block = (carried[0].shape[0] // steps, carried[0].shape[1])
        extra_specs = [pl.BlockSpec(block, lambda i, j, c: (i * nb + j, 0)), pl.BlockSpec(memory_space=pl.ANY)]
        aliases = {2 + 2 * len(a): len(out_shape)}
        out_specs.append(pl.BlockSpec(block, lambda i, j, c: ((1 - c[0]) * steps + i * nb + j, 0)))
        out_shape.append(jax.ShapeDtypeStruct(carried[1].shape, carried[1].dtype))
    return pl.pallas_call(
        functools.partial(wgrad_kernel, len(a), whole_axis is not None, col_sum, bool(carried)),
        grid_spec=pltpu.PrefetchScalarGridSpec(
            num_scalar_prefetch=1, grid=(mb, nb),
            in_specs=[pl.BlockSpec((rows, bm), lambda i, j, c, r=r: (r, i)) for _, r in a]
            + [pl.BlockSpec((rows, bn), lambda i, j, c, r=r: (r, j)) for _, r in b] + extra_specs,
            out_specs=out_specs),
        out_shape=out_shape,
        input_output_aliases=aliases,
        compiler_params=params(2),
        cost_estimate=pl.CostEstimate(flops=2 * len(a) * rows * m * n, bytes_accessed=2 * (len(a) * rows * (m + n) + m * n), transcendentals=0),
        name="wgrad",
    )(core, *[val for val, _ in a], *[val for val, _ in b], *carried)


def place_kernel(core_ref, part_ref, whole_ref, out_ref):
    out_ref[...] = part_ref[...]


def place(part, whole, core, axis):
    bm, bn = 512, 2048
    m, n = part.shape
    if axis == 0:
        out_spec = pl.BlockSpec((bm, bn), lambda i, j, c: ((1 - c[0]) * (m // bm) + i, j))
    else:
        out_spec = pl.BlockSpec((bm, bn), lambda i, j, c: (i, (1 - c[0]) * (n // bn) + j))
    return pl.pallas_call(
        place_kernel,
        grid_spec=pltpu.PrefetchScalarGridSpec(
            num_scalar_prefetch=1, grid=(m // bm, n // bn),
            in_specs=[pl.BlockSpec((bm, bn), lambda i, j, c: (i, j)), pl.BlockSpec(memory_space=pl.ANY)],
            out_specs=out_spec),
        out_shape=jax.ShapeDtypeStruct(whole.shape, whole.dtype),
        input_output_aliases={2: 0},
        compiler_params=params(2),
        cost_estimate=pl.CostEstimate(flops=m * n, bytes_accessed=4 * m * n, transcendentals=0),
        name="place",
    )(core, part, whole)


def join_kernel(dims, extra, core_ref, mine_ref, theirs_ref, w_mine_ref, w_theirs_ref, *rest):
    y = dot(mine_ref[...], w_mine_ref[...], dims) + dot(theirs_ref[...], w_theirs_ref[...], dims)
    if extra:
        y = rest[0][...].astype(jnp.float32) + y + rest[1][...].astype(jnp.float32)
    rest[-1][...] = y.astype(rest[-1].dtype)


def join_heads(mine, theirs, w, core, by_rows, extra=()):
    rows, half = theirs.shape
    bn = 512
    n = w.shape[0 if by_rows else 1]
    act = pl.BlockSpec((rows, half), lambda j, c: (0, 0), pipeline_mode=pl.Buffered(1))
    if by_rows:
        w_specs = [pl.BlockSpec((bn, half), lambda j, c: (j, c[0])), pl.BlockSpec((bn, half), lambda j, c: (j, 1 - c[0]))]
    else:
        w_specs = [pl.BlockSpec((half, bn), lambda j, c: (c[0], j)), pl.BlockSpec((half, bn), lambda j, c: (1 - c[0], j))]
    out_spec = pl.BlockSpec((rows, bn), lambda j, c: (0, j))
    extra_specs = [out_spec, pl.BlockSpec((1, bn), lambda j, c: (0, j))] if extra else []
    return pl.pallas_call(
        functools.partial(join_kernel, NT if by_rows else NN, bool(extra)),
        grid_spec=pltpu.PrefetchScalarGridSpec(
            num_scalar_prefetch=1, grid=(n // bn,), in_specs=[act, act] + w_specs + extra_specs, out_specs=out_spec),
        out_shape=jax.ShapeDtypeStruct((rows, n), jnp.bfloat16 if extra else jnp.float32),
        compiler_params=params(1),
        cost_estimate=pl.CostEstimate(flops=4 * rows * half * n, bytes_accessed=4 * (rows * half + half * n + rows * n), transcendentals=0),
        name="join_heads",
    )(core, mine, theirs, w, w, *extra)


def finish_kernel(y_ref, x_ref, g_ref, gain_ref, dkv_ref, w_kv_ref, out_ref, gain_out_ref):
    d_normed = (y_ref[...] + dot(dkv_ref[...], w_kv_ref[...], NT)).astype(jnp.bfloat16).astype(jnp.float32)
    x_f32 = x_ref[...].astype(jnp.float32)
    scale = lax.rsqrt(jnp.mean(x_f32 * x_f32, axis=1, keepdims=True) + NORM_EPS)
    unit = x_f32 * scale
    d_unit = d_normed * (1.0 + gain_ref[...].astype(jnp.float32))
    dx = scale * (d_unit - unit * jnp.mean(d_unit * unit, axis=1, keepdims=True))
    out_ref[...] = (g_ref[...].astype(jnp.float32) + dx).astype(jnp.bfloat16)

    @pl.when(pl.program_id(0) == 0)
    def _():
        gain_out_ref[...] = jnp.zeros_like(gain_out_ref)

    gain_out_ref[...] += jnp.sum(d_normed * unit, axis=0, keepdims=True)


def finish(y, x, g, gain, dkv, w_kv):
    rows, dim = x.shape
    br = 128
    tile = pl.BlockSpec((br, dim), lambda i: (i, 0))
    line = pl.BlockSpec((1, dim), lambda i: (0, 0))
    return pl.pallas_call(
        finish_kernel,
        grid=(rows // br,),
        in_specs=[tile, tile, tile, line, pl.BlockSpec((br, dkv.shape[1]), lambda i: (i, 0)), resident(w_kv.shape)],
        out_specs=[tile, line],
        out_shape=[jax.ShapeDtypeStruct((rows, dim), jnp.bfloat16), jax.ShapeDtypeStruct((1, dim), jnp.float32)],
        compiler_params=params(1),
        cost_estimate=pl.CostEstimate(flops=2 * rows * dim * dkv.shape[1], bytes_accessed=10 * rows * dim, transcendentals=0),
        name="finish",
    )(y, x, g, gain[None], dkv, w_kv)


def key_cap(k0, first_key, own_key, bk, bq):
    key_idx = k0 + lax.broadcasted_iota(jnp.int32, (bk, bq), 0)
    return jnp.where((key_idx >= first_key) & (key_idx <= own_key), POS_BIG, NEG_BIG)


def block_bounds(first_key, token, bq, bk):
    starts = token.reshape(-1, bq)[:, 0]
    return first_key.reshape(-1, bq)[:, 0] // bk, (starts + bq - 1) // bk + 1, starts


def head_cols(h):
    return slice(h * HEAD_DIM, (h + 1) * HEAD_DIM)


def fwd_kernel(bq, bk, heads, lo_ref, hi_ref, t0_ref, q_ref, k_ref, vt_ref, first_ref, o_ref, lse_ref, m_s, l_s, acc_s):
    i = pl.program_id(0)
    first_key = first_ref[0]
    own_key = t0_ref[i] + lax.broadcasted_iota(jnp.int32, (1, bq), 1)
    m_s[...] = jnp.full_like(m_s, NEG_BIG)
    l_s[...] = jnp.zeros_like(l_s)
    acc_s[...] = jnp.zeros_like(acc_s)

    def body(j, carry):
        k0 = pl.multiple_of(j * bk, bk)
        k_blk = k_ref[pl.ds(k0, bk), :]
        vt_blk = vt_ref[:, pl.ds(k0, bk)]
        cap = key_cap(k0, first_key, own_key, bk, bq)

        def scores(h):
            return dot(k_blk, q_ref[:, head_cols(h)], NT)

        def soften(h, s):
            s = jnp.minimum(s, cap)
            m_old = m_s[h:h + 1]
            m_new = jnp.maximum(m_old, jnp.max(s, axis=0, keepdims=True))
            p = jnp.exp(s - m_new)
            alpha = jnp.exp(m_old - m_new)
            l_s[h:h + 1] = l_s[h:h + 1] * alpha + jnp.sum(p, axis=0, keepdims=True)
            m_s[h:h + 1] = m_new
            return p.astype(jnp.bfloat16), alpha

        def gather_values(h, p, alpha):
            acc_s[h] = acc_s[h] * alpha + dot(vt_blk, p, NN)

        s, held = scores(0), None
        for h in range(heads):
            s_next = scores(h + 1) if h + 1 < heads else None
            now = soften(h, s)
            if held is not None:
                gather_values(h - 1, *held)
            held, s = now, s_next
        gather_values(heads - 1, *held)
        return carry

    lax.fori_loop(lo_ref[i], hi_ref[i], body, 0)
    for h in range(heads):
        l_h = l_s[h:h + 1]
        o_ref[:, head_cols(h)] = (acc_s[h] / l_h).T.astype(jnp.bfloat16)
        lse_ref[0, h:h + 1] = m_s[h:h + 1] + jnp.log(l_h)


def attn_fwd(q, k, vt, first_key, token):
    bq, bk = FWD_BQ, FWD_BK
    tokens, width = q.shape
    heads, nq = width // HEAD_DIM, tokens // bq
    return pl.pallas_call(
        functools.partial(fwd_kernel, bq, bk, heads),
        grid_spec=pltpu.PrefetchScalarGridSpec(
            num_scalar_prefetch=3, grid=(nq,),
            in_specs=[pl.BlockSpec((bq, width), lambda i, *_: (i, 0)), resident(k.shape), resident(vt.shape),
                      pl.BlockSpec((1, 1, bq), lambda i, *_: (i, 0, 0))],
            out_specs=[pl.BlockSpec((bq, width), lambda i, *_: (i, 0)), pl.BlockSpec((1, heads, bq), lambda i, *_: (i, 0, 0))],
            scratch_shapes=[pltpu.VMEM((heads, bq), jnp.float32), pltpu.VMEM((heads, bq), jnp.float32),
                            pltpu.VMEM((heads, HEAD_DIM, bq), jnp.float32)]),
        out_shape=[jax.ShapeDtypeStruct(q.shape, jnp.bfloat16), jax.ShapeDtypeStruct((nq, heads, bq), jnp.float32)],
        compiler_params=params(1),
        cost_estimate=pl.CostEstimate(flops=4 * tokens * width * 2048, bytes_accessed=4 * tokens * width, transcendentals=0),
        name="attn_fwd",
    )(*block_bounds(first_key, token, bq, bk), q, k, vt, first_key.reshape(nq, 1, bq))


def bwd_kernel(bq, bk, heads, add_in, lo_ref, hi_ref, t0_ref, q_ref, do_ref, o_ref, lse_ref, first_ref, cos_ref, sin_ref,
               k_ref, kt_ref, v_ref, *rest):
    dq_ref, dk_ref, dv_ref, dq_s, delta_s = rest[-5:]
    i = pl.program_id(0)

    @pl.when(i == 0)
    def _():
        dk_ref[...] = rest[0][...] if add_in else jnp.zeros_like(dk_ref)
        dv_ref[...] = rest[1][...] if add_in else jnp.zeros_like(dv_ref)

    first_key = first_ref[0]
    own_key = t0_ref[i] + lax.broadcasted_iota(jnp.int32, (1, bq), 1)
    dq_s[...] = jnp.zeros_like(dq_s)
    for h in range(heads):
        row_dot = jnp.sum(do_ref[:, head_cols(h)].astype(jnp.float32) * o_ref[:, head_cols(h)].astype(jnp.float32), axis=1, keepdims=True)
        delta_s[h:h + 1] = jnp.broadcast_to(row_dot, (bq, 128)).T[0:1]

    def body(j, carry):
        k0 = pl.multiple_of(j * bk, bk)
        k_blk = k_ref[pl.ds(k0, bk), :]
        v_blk = v_ref[pl.ds(k0, bk), :]
        kt_blk = kt_ref[:, pl.ds(k0, bk)]
        cap = key_cap(k0, first_key, own_key, bk, bq)
        p_all, ds_all = [], []
        for h in range(heads):
            s = jnp.minimum(dot(k_blk, q_ref[:, head_cols(h)], NT), cap)
            p = jnp.exp(s - lse_ref[0, h:h + 1])
            dp = dot(v_blk, do_ref[:, head_cols(h)], NT)
            ds = (p * (dp - delta_s[h:h + 1])).astype(jnp.bfloat16)
            p_all.append(p.astype(jnp.bfloat16))
            ds_all.append(ds)
            dq_s[h] += dot(kt_blk, ds, NN)
        q_rows = jnp.concatenate([q_ref[:, head_cols(h)] for h in range(heads)], axis=0)
        do_rows = jnp.concatenate([do_ref[:, head_cols(h)] for h in range(heads)], axis=0)
        dv_ref[pl.ds(k0, bk), :] += dot(jnp.concatenate(p_all, axis=1), do_rows, NN)
        dk_ref[pl.ds(k0, bk), :] += dot(jnp.concatenate(ds_all, axis=1), q_rows, NN)
        return carry

    lax.fori_loop(lo_ref[i], hi_ref[i], body, 0)
    cos_t, sin_t = cos_ref[...], sin_ref[...]
    for h in range(heads):
        dq = dq_s[h].astype(jnp.bfloat16).astype(jnp.float32)
        a, b = dq[:ROT_HALF], dq[ROT_HALF:2 * ROT_HALF]
        dq_lin = jnp.concatenate([a * cos_t + b * sin_t, b * cos_t - a * sin_t, dq[2 * ROT_HALF:]], axis=0) * HEAD_DIM ** -0.5
        dq_ref[:, head_cols(h)] = dq_lin.T.astype(jnp.bfloat16)


def attn_bwd(q, d_o, o, lse, k, kt, v, first_key, token, cos_a, sin_a, sums):
    bq, bk = BWD_BQ, BWD_BK
    tokens, width = q.shape
    heads, nq = width // HEAD_DIM, tokens // bq
    lse = lse.transpose(1, 0, 2).reshape(heads, nq, bq).transpose(1, 0, 2)
    tile = pl.BlockSpec((bq, width), lambda i, *_: (i, 0))
    trig = pl.BlockSpec((ROT_HALF, bq), lambda i, *_: (0, i))
    whole_out = pl.BlockSpec(k.shape, lambda i, *_: (0, 0))
    acc_shape = jax.ShapeDtypeStruct(k.shape, jnp.float32)
    return pl.pallas_call(
        functools.partial(bwd_kernel, bq, bk, heads, bool(sums)),
        grid_spec=pltpu.PrefetchScalarGridSpec(
            num_scalar_prefetch=3, grid=(nq,),
            in_specs=[tile, tile, tile, pl.BlockSpec((1, heads, bq), lambda i, *_: (i, 0, 0)),
                      pl.BlockSpec((1, 1, bq), lambda i, *_: (i, 0, 0)), trig, trig]
            + [resident(val.shape) for val in (k, kt, v) + tuple(sums)],
            out_specs=[tile, whole_out, whole_out],
            scratch_shapes=[pltpu.VMEM((heads, HEAD_DIM, bq), jnp.float32), pltpu.VMEM((heads, bq), jnp.float32)]),
        out_shape=[jax.ShapeDtypeStruct(q.shape, jnp.bfloat16), acc_shape, acc_shape],
        compiler_params=params(1),
        cost_estimate=pl.CostEstimate(flops=10 * tokens * width * 2048, bytes_accessed=8 * tokens * width, transcendentals=0),
        name="attn_bwd",
    )(*block_bounds(first_key, token, bq, bk), q, d_o, o, lse, first_key.reshape(nq, 1, bq), cos_a.T, sin_a.T, k, kt, v, *sums)


def solution(mesh):
    row_spec = P("dp", "sp", None)
    tok_spec = P("dp", "sp")
    mat_spec = P(None, None)
    grad_mat = P("dp", None)
    chips_perm = [(0, 2), (1, 3), (2, 0), (3, 1)]
    cores_perm = [(0, 1), (1, 0), (2, 3), (3, 2)]

    def to_chip(val):
        return lax.ppermute(val, "sp", chips_perm)

    def to_core(val):
        return lax.ppermute(val, "sp", cores_perm)

    def local_step(x, seg_ids, positions, out_grad, norm_scale, w_q, w_k, w_v, w_o, b_o):
        x, out_grad = x[0], out_grad[0]
        chunk = x.shape[0]
        me = lax.axis_index("sp")
        core = me % 2
        core_arr = core.astype(jnp.int32).reshape(1)
        pieces = [me, me ^ 1, me ^ 2, me ^ 3]

        def ordered(mine, theirs, axis):
            first = jnp.where(core == 0, mine, theirs)
            second = jnp.where(core == 0, theirs, mine)
            return jnp.concatenate([first, second], axis=axis)

        def piece_rows(val, piece):
            return lax.dynamic_slice_in_dim(val, piece * chunk, chunk, axis=0)

        def pair_rows(val, pair):
            return jnp.concatenate([piece_rows(val, pieces[2 * pair]), piece_rows(val, pieces[2 * pair + 1])], axis=0)

        meta = lax.all_gather(jnp.stack([seg_ids[0], positions[0]]), "sp", axis=1, tiled=True)
        x, out_grad, meta = lax.optimization_barrier((x, out_grad, meta))
        seg_all, pos_all = meta[0], meta[1]
        seq = seg_all.shape[0]
        token = jnp.arange(seq, dtype=jnp.int32)
        is_start = jnp.concatenate([jnp.ones((1,), jnp.bool_), seg_all[1:] != seg_all[:-1]])
        doc_start = lax.cummax(jnp.where(is_start, token, 0))
        first_key = jnp.maximum(doc_start, token - (WINDOW - 1))
        cos_all, sin_all = rope_tables(pos_all)

        n_own = rms_norm(x.astype(jnp.float32), norm_scale.astype(jnp.float32))

        w_kv = jnp.concatenate([w_k, w_v], axis=1)
        kv_lin = dot(n_own, w_kv, NN)
        cos_own, sin_own = piece_rows(cos_all, me), piece_rows(sin_all, me)
        k_own = rotary(kv_lin[:, None, :HEAD_DIM], cos_own, sin_own)[:, 0].astype(jnp.bfloat16)
        kv_own = jnp.concatenate([k_own, kv_lin[:, HEAD_DIM:].astype(jnp.bfloat16)], axis=1)

        kv_2 = to_chip(kv_own)
        n_2 = to_chip(n_own)
        g_2 = to_chip(out_grad)
        n_1, kv_1, g_1 = to_core(n_own), to_core(kv_own), to_core(out_grad)
        kv_3, n_3, g_3 = to_core(kv_2), to_core(n_2), to_core(g_2)
        kv_all = jnp.zeros((seq, 2 * HEAD_DIM), jnp.bfloat16)
        for piece, val in zip(pieces, (kv_own, kv_1, kv_2, kv_3)):
            kv_all = lax.dynamic_update_slice_in_dim(kv_all, val, piece * chunk, axis=0)
        k_all, v_all = kv_all[:, :HEAD_DIM], kv_all[:, HEAD_DIM:]
        kt_all, vt_all = k_all.T, v_all.T

        n_all = [n_own, n_1, n_2, n_3]
        g_all = [out_grad, g_1, g_2, g_3]

        o_all, dq_all = [], []
        kv_sums = ()
        for pair in (0, 1):
            a, b = 2 * pair, 2 * pair + 1
            first_p, token_p = pair_rows(first_key, pair), pair_rows(token, pair)
            cos_p, sin_p = pair_rows(cos_all, pair), pair_rows(sin_all, pair)
            tables = (jnp.concatenate([cos_p, cos_p], axis=1), jnp.concatenate([-sin_p, sin_p], axis=1))
            q = proj_pair(n_all[a], n_all[b], w_q, core_arr, False, tables)
            o, lse = attn_fwd(q, k_all, vt_all, first_p, token_p)
            d_o = proj_pair(g_all[a], g_all[b], w_o, core_arr, True)
            dq, *kv_sums = attn_bwd(q, d_o, o, lse, k_all, kt_all, v_all, first_p, token_p, cos_p, sin_p, kv_sums)
            o_all.append(o)
            dq_all.append(dq)

        block_out = join_heads(o_all[0], to_core(o_all[0][chunk:]), w_o, core_arr, False, (x, b_o[None]))
        d_normed_q = join_heads(dq_all[0], to_core(dq_all[0][chunk:]), w_q, core_arr, True)

        dk, dv = kv_sums
        theirs = to_core(jnp.where(core == 0, dv, dk))
        mine = jnp.where(core == 0, dk, dv) + theirs
        turned = rotary(mine[:, None].astype(jnp.bfloat16).astype(jnp.float32), cos_all, -sin_all)[:, 0]
        mine_lin = jnp.where(core == 0, turned, mine).astype(jnp.bfloat16)
        mine_pieces = [piece_rows(mine_lin, piece) for piece in pieces]

        halves = [(0, 0), (0, 1), (1, 0), (1, 1)]
        w_o_part, w_o_grad, b_o_sum = wgrad([(o_all[i], r) for i, r in halves], [(g, 0) for g in g_all], core_arr, chunk, 512, 1024, 0, True)
        w_o_theirs = to_core(w_o_part)
        w_q_part, w_q_grad, w_o_grad = wgrad([(n, 0) for n in n_all], [(dq_all[i], r) for i, r in halves], core_arr, chunk, 512, 1024, 1,
                                             carried=(w_o_theirs, w_o_grad))
        w_q_theirs = to_core(w_q_part)
        mine_w, = wgrad([(n, 0) for n in n_all], [(val, 0) for val in mine_pieces], core_arr, chunk, 1024, HEAD_DIM)
        theirs_w = to_core(mine_w)
        w_k_grad = jnp.where(core == 0, mine_w, theirs_w)
        w_v_grad = jnp.where(core == 0, theirs_w, mine_w)

        dkv_tok = ordered(mine_pieces[0], to_core(mine_pieces[1]), 1)
        x_grad, gain_part = finish(d_normed_q, x, out_grad, norm_scale, dkv_tok, w_kv)
        w_q_grad = place(w_q_theirs, w_q_grad, core_arr, 1)
        gain_sum = gain_part[0] + to_core(gain_part[0])
        gain_sum = gain_sum + to_chip(gain_sum)
        return (block_out[None], x_grad[None], gain_sum.astype(jnp.bfloat16), w_q_grad, w_k_grad, w_v_grad, w_o_grad,
                b_o_sum[0].astype(jnp.bfloat16))

    return jax.shard_map(local_step, mesh=mesh,
                         in_specs=(row_spec, tok_spec, tok_spec, row_spec, P(None), mat_spec, mat_spec, mat_spec, mat_spec, P(None)),
                         out_specs=(row_spec, row_spec, P("dp"), grad_mat, grad_mat, grad_mat, grad_mat, P("dp")),
                         check_vma=False)
```

```python
import functools

import jax
import jax.numpy as jnp
from jax import lax
from jax.experimental import pallas as pl
from jax.experimental.pallas import tpu as pltpu
from jax.sharding import PartitionSpec as P


WINDOW = 2048
NORM_EPS = 1e-6
ROPE_BASE = 10000.0
NEG_BIG = -1e30
POS_BIG = 3e38
HEAD_DIM = 256
ROT_HALF = HEAD_DIM // 4

FWD_BQ, FWD_BK = 256, 512
BWD_BQ, BWD_BK = 512, 512
VMEM_LIMIT = 67043328

NT = (((1,), (1,)), ((), ()))
NN = (((1,), (0,)), ((), ()))
TN = (((0,), (0,)), ((), ()))


def dot(a, b, dims):
    return lax.dot_general(a, b, dims, preferred_element_type=jnp.float32)


def rms_norm(x_f32, gain_f32):
    mean_sq = jnp.mean(x_f32 * x_f32, axis=-1, keepdims=True)
    return (x_f32 * lax.rsqrt(mean_sq + NORM_EPS) * (1.0 + gain_f32)).astype(jnp.bfloat16)


def rope_tables(positions):
    rot_dim = 2 * ROT_HALF
    inv_freq = ROPE_BASE ** (-(jnp.arange(ROT_HALF, dtype=jnp.float32) * 2.0 / rot_dim))
    angles = positions.astype(jnp.float32)[:, None] * inv_freq
    return jnp.cos(angles), jnp.sin(angles)


def rotary(vals, cos_a, sin_a):
    a = vals[..., :ROT_HALF]
    b = vals[..., ROT_HALF:2 * ROT_HALF]
    cos_a, sin_a = cos_a[:, None, :], sin_a[:, None, :]
    return jnp.concatenate([a * cos_a - b * sin_a, b * cos_a + a * sin_a, vals[..., 2 * ROT_HALF:]], axis=-1)


def resident(shape):
    return pl.BlockSpec(shape, lambda *_: (0,) * len(shape), pipeline_mode=pl.Buffered(1))


def params(axes, **kwargs):
    return pltpu.CompilerParams(dimension_semantics=("arbitrary",) * axes, vmem_limit_bytes=VMEM_LIMIT, **kwargs)


def proj_kernel(dims, rope, core_ref, a0_ref, a1_ref, w_ref, *rest):
    out_ref = rest[-1]
    rows = a0_ref.shape[0]
    for piece, a_ref in enumerate((a0_ref, a1_ref)):
        y = dot(a_ref[...], w_ref[...], dims)
        r = slice(piece * rows, (piece + 1) * rows)
        if not rope:
            out_ref[r, :] = y.astype(jnp.bfloat16)
            continue
        cos_a, sin_a = rest[0][r, :], rest[1][r, :]
        for h in range(y.shape[1] // HEAD_DIM):
            c0, c1, c2 = h * HEAD_DIM, h * HEAD_DIM + 2 * ROT_HALF, (h + 1) * HEAD_DIM
            turned = y[:, c0:c1] * cos_a + pltpu.roll(y[:, c0:c1], ROT_HALF, 1) * sin_a
            out_ref[r, c0:c1] = (turned * HEAD_DIM ** -0.5).astype(jnp.bfloat16)
            out_ref[r, c1:c2] = (y[:, c1:c2] * HEAD_DIM ** -0.5).astype(jnp.bfloat16)


def proj_pair(a0, a1, w, core, by_rows, tables=()):
    rows, depth = a0.shape
    half = w.shape[0 if by_rows else 1] // 2
    bn = 512
    nb = half // bn
    if by_rows:
        w_spec = pl.BlockSpec((bn, depth), lambda j, c: (c[0] * nb + j, 0))
    else:
        w_spec = pl.BlockSpec((depth, bn), lambda j, c: (0, c[0] * nb + j))
    return pl.pallas_call(
        functools.partial(proj_kernel, NT if by_rows else NN, bool(tables)),
        grid_spec=pltpu.PrefetchScalarGridSpec(
            num_scalar_prefetch=1, grid=(nb,),
            in_specs=[resident(a0.shape), resident(a1.shape), w_spec] + [resident(t.shape) for t in tables],
            out_specs=pl.BlockSpec((2 * rows, bn), lambda j, c: (0, j))),
        out_shape=jax.ShapeDtypeStruct((2 * rows, half), jnp.bfloat16),
        compiler_params=params(1),
        cost_estimate=pl.CostEstimate(flops=4 * rows * depth * half, bytes_accessed=2 * (2 * rows * (depth + half) + depth * half), transcendentals=0),
        name="proj_pair",
    )(core, a0, a1, w, *tables)


def wgrad_kernel(pieces, whole, col_sum, carried, core_ref, *refs):
    a_refs, b_refs, outs = refs[:pieces], refs[pieces:2 * pieces], refs[2 * pieces:]
    if carried:
        outs[-1][...] = outs[0][...]
        outs = outs[2:-1]
    y = sum(dot(a[...], b[...], TN) for a, b in zip(a_refs, b_refs)).astype(jnp.bfloat16)
    outs[0][...] = y
    if whole:
        outs[1][...] = y
    if col_sum:
        @pl.when(pl.program_id(0) == 0)
        def _():
            outs[-1][...] = sum(jnp.sum(b[...].astype(jnp.float32), axis=0, keepdims=True) for b in b_refs)


def wgrad(a, b, core, rows, bm, bn, whole_axis=None, col_sum=False, carried=()):
    m, n = a[0][0].shape[1], b[0][0].shape[1]
    mb, nb = m // bm, n // bn
    out_specs = [pl.BlockSpec((bm, bn), lambda i, j, c: (i, j))]
    out_shape = [jax.ShapeDtypeStruct((m, n), jnp.bfloat16)]
    if whole_axis == 0:
        out_specs.append(pl.BlockSpec((bm, bn), lambda i, j, c: (c[0] * mb + i, j)))
        out_shape.append(jax.ShapeDtypeStruct((2 * m, n), jnp.bfloat16))
    if whole_axis == 1:
        out_specs.append(pl.BlockSpec((bm, bn), lambda i, j, c: (i, c[0] * nb + j)))
        out_shape.append(jax.ShapeDtypeStruct((m, 2 * n), jnp.bfloat16))
    if col_sum:
        out_specs.append(pl.BlockSpec((1, bn), lambda i, j, c: (0, jnp.where(i == 0, j, nb - 1))))
        out_shape.append(jax.ShapeDtypeStruct((1, n), jnp.float32))
    extra_specs, aliases = [], {}
    if carried:
        steps = mb * nb
        block = (carried[0].shape[0] // steps, carried[0].shape[1])
        extra_specs = [pl.BlockSpec(block, lambda i, j, c: (i * nb + j, 0)), pl.BlockSpec(memory_space=pl.ANY)]
        aliases = {2 + 2 * len(a): len(out_shape)}
        out_specs.append(pl.BlockSpec(block, lambda i, j, c: ((1 - c[0]) * steps + i * nb + j, 0)))
        out_shape.append(jax.ShapeDtypeStruct(carried[1].shape, carried[1].dtype))
    return pl.pallas_call(
        functools.partial(wgrad_kernel, len(a), whole_axis is not None, col_sum, bool(carried)),
        grid_spec=pltpu.PrefetchScalarGridSpec(
            num_scalar_prefetch=1, grid=(mb, nb),
            in_specs=[pl.BlockSpec((rows, bm), lambda i, j, c, r=r: (r, i)) for _, r in a]
            + [pl.BlockSpec((rows, bn), lambda i, j, c, r=r: (r, j)) for _, r in b] + extra_specs,
            out_specs=out_specs),
        out_shape=out_shape,
        input_output_aliases=aliases,
        compiler_params=params(2),
        cost_estimate=pl.CostEstimate(flops=2 * len(a) * rows * m * n, bytes_accessed=2 * (len(a) * rows * (m + n) + m * n), transcendentals=0),
        name="wgrad",
    )(core, *[val for val, _ in a], *[val for val, _ in b], *carried)


def place_kernel(core_ref, part_ref, whole_ref, out_ref):
    out_ref[...] = part_ref[...]


def place(part, whole, core, axis):
    bm, bn = 512, 2048
    m, n = part.shape
    if axis == 0:
        out_spec = pl.BlockSpec((bm, bn), lambda i, j, c: ((1 - c[0]) * (m // bm) + i, j))
    else:
        out_spec = pl.BlockSpec((bm, bn), lambda i, j, c: (i, (1 - c[0]) * (n // bn) + j))
    return pl.pallas_call(
        place_kernel,
        grid_spec=pltpu.PrefetchScalarGridSpec(
            num_scalar_prefetch=1, grid=(m // bm, n // bn),
            in_specs=[pl.BlockSpec((bm, bn), lambda i, j, c: (i, j)), pl.BlockSpec(memory_space=pl.ANY)],
            out_specs=out_spec),
        out_shape=jax.ShapeDtypeStruct(whole.shape, whole.dtype),
        input_output_aliases={2: 0},
        compiler_params=params(2),
        cost_estimate=pl.CostEstimate(flops=m * n, bytes_accessed=4 * m * n, transcendentals=0),
        name="place",
    )(core, part, whole)


def join_kernel(dims, extra, core_ref, mine_ref, theirs_ref, w_mine_ref, w_theirs_ref, *rest):
    y = dot(mine_ref[...], w_mine_ref[...], dims) + dot(theirs_ref[...], w_theirs_ref[...], dims)
    if extra:
        y = rest[0][...].astype(jnp.float32) + y + rest[1][...].astype(jnp.float32)
    rest[-1][...] = y.astype(rest[-1].dtype)


def join_heads(mine, theirs, w, core, by_rows, extra=()):
    rows, half = theirs.shape
    bn = 512
    n = w.shape[0 if by_rows else 1]
    act = pl.BlockSpec((rows, half), lambda j, c: (0, 0), pipeline_mode=pl.Buffered(1))
    if by_rows:
        w_specs = [pl.BlockSpec((bn, half), lambda j, c: (j, c[0])), pl.BlockSpec((bn, half), lambda j, c: (j, 1 - c[0]))]
    else:
        w_specs = [pl.BlockSpec((half, bn), lambda j, c: (c[0], j)), pl.BlockSpec((half, bn), lambda j, c: (1 - c[0], j))]
    out_spec = pl.BlockSpec((rows, bn), lambda j, c: (0, j))
    extra_specs = [out_spec, pl.BlockSpec((1, bn), lambda j, c: (0, j))] if extra else []
    return pl.pallas_call(
        functools.partial(join_kernel, NT if by_rows else NN, bool(extra)),
        grid_spec=pltpu.PrefetchScalarGridSpec(
            num_scalar_prefetch=1, grid=(n // bn,), in_specs=[act, act] + w_specs + extra_specs, out_specs=out_spec),
        out_shape=jax.ShapeDtypeStruct((rows, n), jnp.bfloat16 if extra else jnp.float32),
        compiler_params=params(1),
        cost_estimate=pl.CostEstimate(flops=4 * rows * half * n, bytes_accessed=4 * (rows * half + half * n + rows * n), transcendentals=0),
        name="join_heads",
    )(core, mine, theirs, w, w, *extra)


def finish_kernel(y_ref, x_ref, g_ref, gain_ref, dkv_ref, w_kv_ref, out_ref, gain_out_ref):
    d_normed = (y_ref[...] + dot(dkv_ref[...], w_kv_ref[...], NT)).astype(jnp.bfloat16).astype(jnp.float32)
    x_f32 = x_ref[...].astype(jnp.float32)
    scale = lax.rsqrt(jnp.mean(x_f32 * x_f32, axis=1, keepdims=True) + NORM_EPS)
    unit = x_f32 * scale
    d_unit = d_normed * (1.0 + gain_ref[...].astype(jnp.float32))
    dx = scale * (d_unit - unit * jnp.mean(d_unit * unit, axis=1, keepdims=True))
    out_ref[...] = (g_ref[...].astype(jnp.float32) + dx).astype(jnp.bfloat16)

    @pl.when(pl.program_id(0) == 0)
    def _():
        gain_out_ref[...] = jnp.zeros_like(gain_out_ref)

    gain_out_ref[...] += jnp.sum(d_normed * unit, axis=0, keepdims=True)


def finish(y, x, g, gain, dkv, w_kv):
    rows, dim = x.shape
    br = 128
    tile = pl.BlockSpec((br, dim), lambda i: (i, 0))
    line = pl.BlockSpec((1, dim), lambda i: (0, 0))
    return pl.pallas_call(
        finish_kernel,
        grid=(rows // br,),
        in_specs=[tile, tile, tile, line, pl.BlockSpec((br, dkv.shape[1]), lambda i: (i, 0)), resident(w_kv.shape)],
        out_specs=[tile, line],
        out_shape=[jax.ShapeDtypeStruct((rows, dim), jnp.bfloat16), jax.ShapeDtypeStruct((1, dim), jnp.float32)],
        compiler_params=params(1),
        cost_estimate=pl.CostEstimate(flops=2 * rows * dim * dkv.shape[1], bytes_accessed=10 * rows * dim, transcendentals=0),
        name="finish",
    )(y, x, g, gain[None], dkv, w_kv)


def key_cap(k0, first_key, own_key, bk, bq):
    key_idx = k0 + lax.broadcasted_iota(jnp.int32, (bk, bq), 0)
    return jnp.where((key_idx >= first_key) & (key_idx <= own_key), POS_BIG, NEG_BIG)


def block_bounds(first_key, token, bq, bk):
    starts = token.reshape(-1, bq)[:, 0]
    return first_key.reshape(-1, bq)[:, 0] // bk, (starts + bq - 1) // bk + 1, starts


def head_cols(h):
    return slice(h * HEAD_DIM, (h + 1) * HEAD_DIM)


def fwd_kernel(bq, bk, heads, lo_ref, hi_ref, t0_ref, q_ref, k_ref, vt_ref, first_ref, o_ref, lse_ref, m_s, l_s, acc_s):
    i = pl.program_id(0)
    first_key = first_ref[0]
    own_key = t0_ref[i] + lax.broadcasted_iota(jnp.int32, (1, bq), 1)
    m_s[...] = jnp.full_like(m_s, NEG_BIG)
    l_s[...] = jnp.zeros_like(l_s)
    acc_s[...] = jnp.zeros_like(acc_s)

    def body(j, carry):
        k0 = pl.multiple_of(j * bk, bk)
        k_blk = k_ref[pl.ds(k0, bk), :]
        vt_blk = vt_ref[:, pl.ds(k0, bk)]
        cap = key_cap(k0, first_key, own_key, bk, bq)

        def scores(h):
            return dot(k_blk, q_ref[:, head_cols(h)], NT)

        def soften(h, s):
            s = jnp.minimum(s, cap)
            m_old = m_s[h:h + 1]
            m_new = jnp.maximum(m_old, jnp.max(s, axis=0, keepdims=True))
            p = jnp.exp(s - m_new)
            alpha = jnp.exp(m_old - m_new)
            l_s[h:h + 1] = l_s[h:h + 1] * alpha + jnp.sum(p, axis=0, keepdims=True)
            m_s[h:h + 1] = m_new
            return p.astype(jnp.bfloat16), alpha

        def gather_values(h, p, alpha):
            acc_s[h] = acc_s[h] * alpha + dot(vt_blk, p, NN)

        s, held = scores(0), None
        for h in range(heads):
            s_next = scores(h + 1) if h + 1 < heads else None
            now = soften(h, s)
            if held is not None:
                gather_values(h - 1, *held)
            held, s = now, s_next
        gather_values(heads - 1, *held)
        return carry

    lax.fori_loop(lo_ref[i], hi_ref[i], body, 0)
    for h in range(heads):
        l_h = l_s[h:h + 1]
        o_ref[:, head_cols(h)] = (acc_s[h] / l_h).T.astype(jnp.bfloat16)
        lse_ref[0, h:h + 1] = m_s[h:h + 1] + jnp.log(l_h)


def attn_fwd(q, k, vt, first_key, token):
    bq, bk = FWD_BQ, FWD_BK
    tokens, width = q.shape
    heads, nq = width // HEAD_DIM, tokens // bq
    return pl.pallas_call(
        functools.partial(fwd_kernel, bq, bk, heads),
        grid_spec=pltpu.PrefetchScalarGridSpec(
            num_scalar_prefetch=3, grid=(nq,),
            in_specs=[pl.BlockSpec((bq, width), lambda i, *_: (i, 0)), resident(k.shape), resident(vt.shape),
                      pl.BlockSpec((1, 1, bq), lambda i, *_: (i, 0, 0))],
            out_specs=[pl.BlockSpec((bq, width), lambda i, *_: (i, 0)), pl.BlockSpec((1, heads, bq), lambda i, *_: (i, 0, 0))],
            scratch_shapes=[pltpu.VMEM((heads, bq), jnp.float32), pltpu.VMEM((heads, bq), jnp.float32),
                            pltpu.VMEM((heads, HEAD_DIM, bq), jnp.float32)]),
        out_shape=[jax.ShapeDtypeStruct(q.shape, jnp.bfloat16), jax.ShapeDtypeStruct((nq, heads, bq), jnp.float32)],
        compiler_params=params(1),
        cost_estimate=pl.CostEstimate(flops=4 * tokens * width * 2048, bytes_accessed=4 * tokens * width, transcendentals=0),
        name="attn_fwd",
    )(*block_bounds(first_key, token, bq, bk), q, k, vt, first_key.reshape(nq, 1, bq))


def bwd_kernel(bq, bk, heads, add_in, lo_ref, hi_ref, t0_ref, q_ref, do_ref, o_ref, lse_ref, first_ref, cos_ref, sin_ref,
               k_ref, kt_ref, v_ref, *rest):
    dq_ref, dk_ref, dv_ref, dq_s, delta_s = rest[-5:]
    i = pl.program_id(0)

    @pl.when(i == 0)
    def _():
        dk_ref[...] = rest[0][...] if add_in else jnp.zeros_like(dk_ref)
        dv_ref[...] = rest[1][...] if add_in else jnp.zeros_like(dv_ref)

    first_key = first_ref[0]
    own_key = t0_ref[i] + lax.broadcasted_iota(jnp.int32, (1, bq), 1)
    dq_s[...] = jnp.zeros_like(dq_s)
    for h in range(heads):
        row_dot = jnp.sum(do_ref[:, head_cols(h)].astype(jnp.float32) * o_ref[:, head_cols(h)].astype(jnp.float32), axis=1, keepdims=True)
        delta_s[h:h + 1] = jnp.broadcast_to(row_dot, (bq, 128)).T[0:1]

    def body(j, carry):
        k0 = pl.multiple_of(j * bk, bk)
        k_blk = k_ref[pl.ds(k0, bk), :]
        v_blk = v_ref[pl.ds(k0, bk), :]
        kt_blk = kt_ref[:, pl.ds(k0, bk)]
        cap = key_cap(k0, first_key, own_key, bk, bq)
        p_all, ds_all = [], []
        for h in range(heads):
            s = jnp.minimum(dot(k_blk, q_ref[:, head_cols(h)], NT), cap)
            p = jnp.exp(s - lse_ref[0, h:h + 1])
            dp = dot(v_blk, do_ref[:, head_cols(h)], NT)
            ds = (p * (dp - delta_s[h:h + 1])).astype(jnp.bfloat16)
            p_all.append(p.astype(jnp.bfloat16))
            ds_all.append(ds)
            dq_s[h] += dot(kt_blk, ds, NN)
        q_rows = jnp.concatenate([q_ref[:, head_cols(h)] for h in range(heads)], axis=0)
        do_rows = jnp.concatenate([do_ref[:, head_cols(h)] for h in range(heads)], axis=0)
        dv_ref[pl.ds(k0, bk), :] += dot(jnp.concatenate(p_all, axis=1), do_rows, NN)
        dk_ref[pl.ds(k0, bk), :] += dot(jnp.concatenate(ds_all, axis=1), q_rows, NN)
        return carry

    lax.fori_loop(lo_ref[i], hi_ref[i], body, 0)
    cos_t, sin_t = cos_ref[...], sin_ref[...]
    for h in range(heads):
        dq = dq_s[h].astype(jnp.bfloat16).astype(jnp.float32)
        a, b = dq[:ROT_HALF], dq[ROT_HALF:2 * ROT_HALF]
        dq_lin = jnp.concatenate([a * cos_t + b * sin_t, b * cos_t - a * sin_t, dq[2 * ROT_HALF:]], axis=0) * HEAD_DIM ** -0.5
        dq_ref[:, head_cols(h)] = dq_lin.T.astype(jnp.bfloat16)


def attn_bwd(q, d_o, o, lse, k, kt, v, first_key, token, cos_a, sin_a, sums):
    bq, bk = BWD_BQ, BWD_BK
    tokens, width = q.shape
    heads, nq = width // HEAD_DIM, tokens // bq
    lse = lse.transpose(1, 0, 2).reshape(heads, nq, bq).transpose(1, 0, 2)
    tile = pl.BlockSpec((bq, width), lambda i, *_: (i, 0))
    trig = pl.BlockSpec((ROT_HALF, bq), lambda i, *_: (0, i))
    whole_out = pl.BlockSpec(k.shape, lambda i, *_: (0, 0))
    acc_shape = jax.ShapeDtypeStruct(k.shape, jnp.float32)
    return pl.pallas_call(
        functools.partial(bwd_kernel, bq, bk, heads, bool(sums)),
        grid_spec=pltpu.PrefetchScalarGridSpec(
            num_scalar_prefetch=3, grid=(nq,),
            in_specs=[tile, tile, tile, pl.BlockSpec((1, heads, bq), lambda i, *_: (i, 0, 0)),
                      pl.BlockSpec((1, 1, bq), lambda i, *_: (i, 0, 0)), trig, trig]
            + [resident(val.shape) for val in (k, kt, v) + tuple(sums)],
            out_specs=[tile, whole_out, whole_out],
            scratch_shapes=[pltpu.VMEM((heads, HEAD_DIM, bq), jnp.float32), pltpu.VMEM((heads, bq), jnp.float32)]),
        out_shape=[jax.ShapeDtypeStruct(q.shape, jnp.bfloat16), acc_shape, acc_shape],
        compiler_params=params(1),
        cost_estimate=pl.CostEstimate(flops=10 * tokens * width * 2048, bytes_accessed=8 * tokens * width, transcendentals=0),
        name="attn_bwd",
    )(*block_bounds(first_key, token, bq, bk), q, d_o, o, lse, first_key.reshape(nq, 1, bq), cos_a.T, sin_a.T, k, kt, v, *sums)


def solution(mesh):
    row_spec = P("dp", "sp", None)
    tok_spec = P("dp", "sp")
    mat_spec = P(None, None)
    grad_mat = P("dp", None)
    chips_perm = [(0, 2), (1, 3), (2, 0), (3, 1)]
    cores_perm = [(0, 1), (1, 0), (2, 3), (3, 2)]

    def to_chip(val, perm=tuple(chips_perm)):
        return lax.ppermute(val, "sp", perm)

    def to_core(val):
        return lax.ppermute(val, "sp", cores_perm)

    def local_step(x, seg_ids, positions, out_grad, norm_scale, w_q, w_k, w_v, w_o, b_o):
        x, out_grad = x[0], out_grad[0]
        chunk = x.shape[0]
        me = lax.axis_index("sp")
        core = me % 2
        core_arr = core.astype(jnp.int32).reshape(1)
        pieces = [me, me ^ 1, me ^ 2, me ^ 3]

        def ordered(mine, theirs, axis):
            first = jnp.where(core == 0, mine, theirs)
            second = jnp.where(core == 0, theirs, mine)
            return jnp.concatenate([first, second], axis=axis)

        def piece_rows(val, piece):
            return lax.dynamic_slice_in_dim(val, piece * chunk, chunk, axis=0)

        def pair_rows(val, pair):
            return jnp.concatenate([piece_rows(val, pieces[2 * pair]), piece_rows(val, pieces[2 * pair + 1])], axis=0)

        meta = lax.all_gather(jnp.stack([seg_ids[0], positions[0]]), "sp", axis=1, tiled=True)
        x, out_grad, meta = lax.optimization_barrier((x, out_grad, meta))
        seg_all, pos_all = meta[0], meta[1]
        seq = seg_all.shape[0]
        token = jnp.arange(seq, dtype=jnp.int32)
        is_start = jnp.concatenate([jnp.ones((1,), jnp.bool_), seg_all[1:] != seg_all[:-1]])
        doc_start = lax.cummax(jnp.where(is_start, token, 0))
        first_key = jnp.maximum(doc_start, token - (WINDOW - 1))
        cos_all, sin_all = rope_tables(pos_all)

        n_own = rms_norm(x.astype(jnp.float32), norm_scale.astype(jnp.float32))

        w_kv = jnp.concatenate([w_k, w_v], axis=1)
        kv_lin = dot(n_own, w_kv, NN)
        cos_own, sin_own = piece_rows(cos_all, me), piece_rows(sin_all, me)
        k_own = rotary(kv_lin[:, None, :HEAD_DIM], cos_own, sin_own)[:, 0].astype(jnp.bfloat16)
        kv_own = jnp.concatenate([k_own, kv_lin[:, HEAD_DIM:].astype(jnp.bfloat16)], axis=1)

        kv_2 = to_chip(kv_own)
        n_2 = to_chip(n_own)
        g_2 = to_chip(out_grad)
        n_1, kv_1, g_1 = to_core(n_own), to_core(kv_own), to_core(out_grad)
        kv_3, n_3, g_3 = to_core(kv_2), to_core(n_2), to_core(g_2)
        kv_all = jnp.zeros((seq, 2 * HEAD_DIM), jnp.bfloat16)
        for piece, val in zip(pieces, (kv_own, kv_1, kv_2, kv_3)):
            kv_all = lax.dynamic_update_slice_in_dim(kv_all, val, piece * chunk, axis=0)
        k_all, v_all = kv_all[:, :HEAD_DIM], kv_all[:, HEAD_DIM:]
        kt_all, vt_all = k_all.T, v_all.T

        n_all = [n_own, n_1, n_2, n_3]
        g_all = [out_grad, g_1, g_2, g_3]

        o_all = []
        for pair in (0, 1):
            a, b = 2 * pair, 2 * pair + 1
            first_p, token_p = pair_rows(first_key, pair), pair_rows(token, pair)
            cos_p, sin_p = pair_rows(cos_all, pair), pair_rows(sin_all, pair)
            tables = (jnp.concatenate([cos_p, cos_p], axis=1), jnp.concatenate([-sin_p, sin_p], axis=1))
            q = proj_pair(n_all[a], n_all[b], w_q, core_arr, False, tables)
            o, lse = attn_fwd(q, k_all, vt_all, first_p, token_p)
            o_all.append(o)
            if pair:
                continue
            d_o = proj_pair(g_all[a], g_all[b], w_o, core_arr, True)
            dq_own, dk, dv = attn_bwd(q, d_o, o, lse, k_all, kt_all, v_all, first_p, token_p, cos_p, sin_p, ())

        block_out = join_heads(o_all[0], to_core(o_all[0][chunk:]), w_o, core_arr, False, (x, b_o[None]))
        dq_theirs = to_core(dq_own[chunk:])
        d_normed_q = join_heads(dq_own, dq_theirs, w_q, core_arr, True)

        pair_len = 2 * chunk
        chip = me // 2

        def chip_rows(val, which):
            return lax.dynamic_slice_in_dim(val, which * pair_len, pair_len, axis=0)

        theirs = to_core(jnp.where(core == 0, dv, dk))
        part = jnp.where(core == 0, dk, dv) + theirs
        dq_other = to_chip(dq_own)
        mine = chip_rows(part, chip) + to_chip(chip_rows(part, 1 - chip), ((2, 0), (3, 1)))
        turned = rotary(mine[:, None].astype(jnp.bfloat16).astype(jnp.float32), chip_rows(cos_all, chip), -chip_rows(sin_all, chip))[:, 0]
        mine_lin = jnp.where(core == 0, turned, mine).astype(jnp.bfloat16)
        other_lin = to_chip(mine_lin)
        mine_pieces = [lax.dynamic_slice_in_dim(val, which * chunk, chunk, axis=0) for val in (mine_lin, other_lin) for which in (core, 1 - core)]

        halves = [(0, 0), (0, 1), (1, 0), (1, 1)]
        w_o_part, w_o_grad, b_o_sum = wgrad([(o_all[i], r) for i, r in halves], [(g, 0) for g in g_all], core_arr, chunk, 512, 1024, 0, True)
        w_o_theirs = to_core(w_o_part)
        w_q_part, w_q_grad, w_o_grad = wgrad([(n, 0) for n in n_all], [((dq_own, dq_other)[i], r) for i, r in halves], core_arr, chunk, 512, 1024, 1,
                                             carried=(w_o_theirs, w_o_grad))
        w_q_theirs = to_core(w_q_part)
        mine_w, = wgrad([(n, 0) for n in n_all], [(val, 0) for val in mine_pieces], core_arr, chunk, 1024, HEAD_DIM)
        theirs_w = to_core(mine_w)
        w_k_grad = jnp.where(core == 0, mine_w, theirs_w)
        w_v_grad = jnp.where(core == 0, theirs_w, mine_w)

        lin_theirs = to_core(mine_pieces[1])
        dkv_tok = ordered(mine_pieces[0], lin_theirs, 1)
        x_grad, gain_part = finish(d_normed_q, x, out_grad, norm_scale, dkv_tok, w_kv)
        w_q_grad = place(w_q_theirs, w_q_grad, core_arr, 1)
        gain_sum = gain_part[0] + to_core(gain_part[0])
        gain_sum = gain_sum + to_chip(gain_sum)
        return (block_out[None], x_grad[None], gain_sum.astype(jnp.bfloat16), w_q_grad, w_k_grad, w_v_grad, w_o_grad,
                b_o_sum[0].astype(jnp.bfloat16))

    return jax.shard_map(local_step, mesh=mesh,
                         in_specs=(row_spec, tok_spec, tok_spec, row_spec, P(None), mat_spec, mat_spec, mat_spec, mat_spec, P(None)),
                         out_specs=(row_spec, row_spec, P("dp"), grad_mat, grad_mat, grad_mat, grad_mat, P("dp")),
                         check_vma=False)
```
